32 devices in a mesh: dp: 8 (over y, x, core), expert: 4 (over z).
Axes of the slice: x: 2, y: 2, z: 4, core: 2. Of those that a mesh axis runs over, the one named last changes fastest.
Arguments:
- tokens: bfloat16 [4096, 2048], P(('dp', 'expert')), may hold values from -6 to 6
- cotangent: bfloat16 [4096, 2048], P(('dp', 'expert')), may hold values from -6 to 6
- expert_ids: int32 [4096, 2], P(('dp', 'expert')), may hold values from 0 to 3, all different within a row; in each aligned block of 128 rows (0 to 127, 128 to 255, ...) at most 128 rows name the same one
- combine: float32 [4096, 2], P(('dp', 'expert')), may hold values from 0.1 to 1
- w_gate: bfloat16 [4, 2048, 768], P('expert'), may hold values from -0.125 to 0.125
- w_up: bfloat16 [4, 2048, 768], P('expert'), may hold values from -0.125 to 0.125
- w_down: bfloat16 [4, 768, 2048], P('expert'), may hold values from -0.21875 to 0.21875
Outputs:
- input_grad: bfloat16 [4096, 2048], P(('dp', 'expert'))
- combine_grad: float32 [4096, 2], P(('dp', 'expert'))
- gate_grad: bfloat16 [4, 2048, 768], P('expert', 'dp')
- up_grad: bfloat16 [4, 2048, 768], P('expert', 'dp')
- down_grad: bfloat16 [4, 768, 2048], P('expert', 'dp')
The draws below stay inside these ranges and needn't reach their ends.
Inputs may be any that keep to these rules, and one draw needn't show every extreme that they name: `expert_ids`: each token names 2 different experts. In the rows of one device no expert is named by more than 128 tokens, and in some devices' rows some expert is named by exactly 128.
All inputs are finite; a program needn't handle non-finite values.
Results may differ from the reference program's by a relative error of at most 0.02.
Values may be sent and summed in bfloat16 or wider, within the bound.
No kernel may reach another device: no remote copies, remote signals or barrier semaphores. Data moves between devices by JAX's collectives and lax.ppermute only.
A program may use at most 128 MiB of HBM per device.

```python
import math
import jax
import jax.numpy as jnp
import numpy as np
from jax import lax

D = 2048
FF = 768
TOK_DEV = 128
TOP = 2
EXPERTS = 4
CAP = 128
TOKENS = 4096
N_DP = 8
N_EXPERT = 4


def steps_of(own_key, shape, split, smallest, largest):
    gain, own = 1.0, jax.random.fold_in(own_key, 6)
    for axis_at, parts in split:
        heights = jnp.exp(jax.random.uniform(jax.random.fold_in(own, axis_at), (parts,), jnp.float32, smallest / len(split), largest / len(split)))
        gain = gain * jnp.repeat(heights, shape[axis_at] // parts).reshape([-1 if axis == axis_at else 1 for axis in range(len(shape))])
    return gain


def deal_out(own_key, own, number, rows, number_of, top, bound, skew):
    ranking = jax.random.permutation(own_key, number_of)
    crowded, common = load_shares(number_of, rows * top, bound, skew, True), load_shares(number_of, rows * top, bound, skew, False)
    places = jnp.arange(number_of)

    def named(lengths, offset_by):
        used = int((lengths > 0).sum())
        fixed = max(1, used // 4)
        shifted = fixed + (places - fixed + offset_by * (used - fixed)) % max(1, number_of - fixed)
        return jnp.zeros((number_of,), jnp.int32).at[ranking[jnp.where(places < fixed, places, shifted)]].set(jnp.asarray(lengths, jnp.int32))

    lengths = jnp.where(number % 4 == 0, named(crowded, number // 4), named(common, number - number // 4 - 1))
    mixed = jax.random.permutation(jax.random.fold_in(own, 3), number_of)
    donor, taker = mixed[0:number_of // 2 * 2:2], mixed[1:number_of // 2 * 2:2]
    room = jnp.minimum(lengths[donor] - 1, bound - lengths[taker]) // 2
    room = jnp.where((donor == ranking[0]) | (taker == ranking[0]) | (lengths[taker] == 0), 0, jnp.maximum(room, 0))
    shifted = jax.random.randint(jax.random.fold_in(own, 4), (number_of // 2,), 0, 1 << 20) % (room + 1)
    lengths = lengths.at[donor].add(-shifted).at[taker].add(shifted)
    items = jnp.searchsorted(jnp.cumsum(lengths), jnp.arange(rows * top), side="right").astype(jnp.int32)
    listing = items.reshape(top, rows).T
    listing = listing[jax.random.permutation(jax.random.fold_in(own, 1), rows)]
    offset_by = jax.random.randint(jax.random.fold_in(own, 2), (rows, 1), 0, top)
    return jnp.take_along_axis(listing, (jnp.arange(top)[None, :] + offset_by) % top, axis=1)


def load_shares(number_of, total, bound, skew, full):
    weights = [(1 << 20) // math.isqrt(standing ** skew) + 1 for standing in range(1, number_of + 1)]
    largest = bound if full else min(bound, max(-(-total // number_of), total * weights[0] // sum(weights)))
    least = 1 if total - largest >= number_of - 1 else 0
    holding, spare = [largest] + [least] * (number_of - 1), total - largest - least * (number_of - 1)
    while spare > 0:
        candidates = [i for i in range(1, number_of) if holding[i] < largest] or [i for i in range(1, number_of) if holding[i] < bound]
        mass, left = sum([weights[i] for i in candidates]), spare
        for i in candidates:
            more = min(bound - holding[i], max(1, left * weights[i] // mass), spare)
            holding[i] = holding[i] + more
            spare = spare - more
    return np.array(holding)


def noise(rng, shape, deviation, reach, split=(), kind=jnp.bfloat16):
    result = jax.random.normal(rng, shape, jnp.float32) * deviation
    if len(split) > 0:
        result = steps_of(rng, shape, split, -0.22, 0.18) * result
    return jnp.clip(result, min=-reach, max=reach).astype(kind)


def setup_inputs(seed: int = 0) -> dict:
    key_list = jax.random.split(jax.random.key(seed), 8)
    tokens = noise(key_list[0], (TOKENS, D), 1.0, 6.0, ((0, 32),))
    cotangent = noise(key_list[1], (TOKENS, D), 1.0, 6.0, ((0, 32),))
    expert_ids_keys = jax.random.split(jax.random.fold_in(key_list[2], 1), TOKENS // TOK_DEV)
    expert_ids_turns = jax.random.permutation(jax.random.fold_in(key_list[2], 3), TOKENS // TOK_DEV)
    expert_ids = jax.vmap(lambda own, number: deal_out(jax.random.fold_in(key_list[2], 2), own, number, TOK_DEV, EXPERTS, TOP, CAP, 2))(expert_ids_keys, expert_ids_turns).reshape((TOKENS, TOP))
    combine = jnp.clip(jnp.exp(math.log(1.0) - 2.3025851 * jax.random.uniform(key_list[3], (TOKENS, TOP), jnp.float32) ** steps_of(key_list[3], (TOKENS, TOP), ((0, 32),), -0.2, 0.2)), 0.1, 1.0)
    w_gate = noise(key_list[4], (EXPERTS, D, FF), D ** -0.5, 0.125, ((0, 4),))
    w_up = noise(key_list[5], (EXPERTS, D, FF), D ** -0.5, 0.125, ((0, 4),))
    w_down = noise(key_list[6], (EXPERTS, FF, D), FF ** -0.5, 0.21875, ((0, 4),))
    return dict(tokens=tokens, cotangent=cotangent, expert_ids=expert_ids, combine=combine, w_gate=w_gate, w_up=w_up, w_down=w_down)


def slot_table(expert_ids, experts_all, capacity):
    pairs = expert_ids.reshape(-1).astype(jnp.int32)
    count = pairs.shape[0]
    onehot = (pairs[:, None] == jnp.arange(experts_all, dtype=jnp.int32)[None, :]).astype(jnp.int32)
    before = jnp.cumsum(onehot, axis=0) - onehot
    position = jnp.sum(before * onehot, axis=1).astype(jnp.int32)
    dest = (pairs * capacity + position).astype(jnp.int32)
    filled = jnp.zeros((experts_all * capacity,), jnp.int32).at[dest].set(jnp.arange(count, dtype=jnp.int32) + 1)
    return dest, filled


def gather_rows(tokens, cotangent, combine, filled, top):
    live = filled > 0
    pair = jnp.maximum(filled - 1, 0).astype(jnp.int32)
    source = (pair // top).astype(jnp.int32)
    rows_x = jnp.where(live[:, None], jnp.take(tokens, source, axis=0), jnp.zeros((), tokens.dtype))
    rows_dy = jnp.where(live[:, None], jnp.take(cotangent, source, axis=0), jnp.zeros((), cotangent.dtype))
    rows_c = jnp.where(live, jnp.take(combine.reshape(-1), pair, axis=0), jnp.zeros((), combine.dtype))
    return rows_x, rows_dy, rows_c


def forward_part(rows_x, gate_mat, up_mat, down_mat):
    gate = jnp.dot(rows_x, gate_mat, preferred_element_type=jnp.float32)
    up = jnp.dot(rows_x, up_mat, preferred_element_type=jnp.float32)
    sig = jax.nn.sigmoid(gate)
    act = gate * sig
    hidden = (act * up).astype(jnp.bfloat16)
    output = jnp.dot(hidden, down_mat, preferred_element_type=jnp.float32)
    return gate, up, sig, act, hidden, output


def backward_part(state, rows_dy, rows_c, gate_mat, up_mat, down_mat):
    gate, up, sig, act, hidden, output = state
    comb_grad = jnp.sum(rows_dy.astype(jnp.float32) * output, axis=1)
    scaled = (rows_c[:, None] * rows_dy.astype(jnp.float32)).astype(jnp.bfloat16)
    last = (((1,), (1,)), ((), ()))
    hidden_grad = lax.dot_general(scaled, down_mat, last, preferred_element_type=jnp.float32)
    gate_d = (hidden_grad * up * (sig * (1.0 + gate * (1.0 - sig)))).astype(jnp.bfloat16)
    up_d = (hidden_grad * act).astype(jnp.bfloat16)
    row_grad = lax.dot_general(gate_d, gate_mat, last, preferred_element_type=jnp.float32)
    row_grad = (row_grad + lax.dot_general(up_d, up_mat, last, preferred_element_type=jnp.float32)).astype(jnp.bfloat16)
    return comb_grad, scaled, gate_d, up_d, row_grad


def reference(tokens, cotangent, expert_ids, combine, w_gate, w_up, w_down):
    first = (((0,), (0,)), ((), ()))
    x_all = tokens.reshape(N_DP, N_EXPERT, TOK_DEV, D)
    dy_all = cotangent.reshape(N_DP, N_EXPERT, TOK_DEV, D)
    id_all = expert_ids.reshape(N_DP, N_EXPERT, TOK_DEV, TOP)
    c_all = combine.reshape(N_DP, N_EXPERT, TOK_DEV, TOP)

    def prepare(x_q, dy_q, id_q, c_q):
        dest, filled = slot_table(id_q, EXPERTS, CAP)
        rows_x, rows_dy, rows_c = gather_rows(x_q, dy_q, c_q, filled, TOP)
        return dest, rows_x.reshape(EXPERTS, CAP, D), rows_dy.reshape(EXPERTS, CAP, D), rows_c.reshape(EXPERTS, CAP)

    def one_expert(item):
        inputs, cot_rows, comb_rows, gate_mat, up_mat, down_mat = item
        state = forward_part(inputs, gate_mat, up_mat, down_mat)
        comb_grad, scaled, gate_d, up_d, row_grad = backward_part(state, cot_rows, comb_rows, gate_mat, up_mat, down_mat)
        gate_part = lax.dot_general(inputs, gate_d, first, preferred_element_type=jnp.float32).astype(jnp.bfloat16)
        up_part = lax.dot_general(inputs, up_d, first, preferred_element_type=jnp.float32).astype(jnp.bfloat16)
        down_part = lax.dot_general(state[4], scaled, first, preferred_element_type=jnp.float32).astype(jnp.bfloat16)
        return row_grad, comb_grad, gate_part, up_part, down_part

    def finish(flat_rows, flat_comb, dest):
        picked = jnp.take(flat_rows, dest, axis=0).reshape(TOK_DEV, TOP, D)
        summed = jnp.sum(picked.astype(jnp.float32), axis=1).astype(jnp.bfloat16)
        return summed, jnp.take(flat_comb, dest, axis=0).reshape(TOK_DEV, TOP)

    def one_replica(carry, inputs):
        x_r, dy_r, id_r, c_r = inputs
        dest, rx, rdy, rc = jax.vmap(prepare)(x_r, dy_r, id_r, c_r)
        group_x = jnp.transpose(rx, (1, 0, 2, 3)).reshape(EXPERTS, N_EXPERT * CAP, D)
        group_dy = jnp.transpose(rdy, (1, 0, 2, 3)).reshape(EXPERTS, N_EXPERT * CAP, D)
        group_c = jnp.transpose(rc, (1, 0, 2)).reshape(EXPERTS, N_EXPERT * CAP)
        rows, combs, gate_part, up_part, down_part = lax.map(one_expert, (group_x, group_dy, group_c, w_gate, w_up, w_down))
        gate_part, up_part, down_part = lax.optimization_barrier((gate_part, up_part, down_part))
        carry = (carry[0] + gate_part.astype(jnp.float32), carry[1] + up_part.astype(jnp.float32), carry[2] + down_part.astype(jnp.float32))
        back = jnp.transpose(rows.reshape(EXPERTS, N_EXPERT, CAP, D), (1, 0, 2, 3)).reshape(N_EXPERT, EXPERTS * CAP, D)
        back_c = jnp.transpose(combs.reshape(EXPERTS, N_EXPERT, CAP), (1, 0, 2)).reshape(N_EXPERT, EXPERTS * CAP)
        grads_in, grads_c = jax.vmap(finish)(back, back_c, dest)
        return carry, (grads_in, grads_c)

    start = (jnp.zeros((EXPERTS, D, FF), jnp.float32), jnp.zeros((EXPERTS, D, FF), jnp.float32), jnp.zeros((EXPERTS, FF, D), jnp.float32))
    sums, (grads_in, grads_c) = lax.scan(one_replica, start, (x_all, dy_all, id_all, c_all))
    input_grad = grads_in.reshape(TOKENS, D)
    combine_grad = grads_c.reshape(TOKENS, TOP)
    return (input_grad, combine_grad, sums[0].astype(jnp.bfloat16), sums[1].astype(jnp.bfloat16), sums[2].astype(jnp.bfloat16))
```

```python
import jax
import jax.numpy as jnp
from jax import lax
from jax.sharding import PartitionSpec as P

LAST = (((1,), (1,)), ((), ()))
FIRST = (((0,), (0,)), ((), ()))


def ring_blocks(own, groups):
    ring = [(i, (i + 1) % groups) for i in range(groups)]
    blocks = [own]
    for _ in range(groups - 1):
        blocks.append(lax.ppermute(blocks[-1], "expert", ring))
    return blocks


def halve(part, bit, replicas):
    pairs = [(i, i ^ (1 << bit)) for i in range(replicas)]
    mine = (lax.axis_index("dp") >> bit) & 1
    send = lax.dynamic_index_in_dim(part, 1 - mine, 0, keepdims=False)
    keep = lax.dynamic_index_in_dim(part, mine, 0, keepdims=False)
    got = lax.ppermute(send, "dp", pairs)
    return (keep.astype(jnp.float32) + got.astype(jnp.float32)).astype(jnp.bfloat16)


def scatter_sum(part, order, replicas):
    rows, columns = part.shape
    bits = len(order)
    part = part.reshape((2,) * bits + (rows // replicas, columns))
    left = list(range(bits - 1, -1, -1))
    for bit in order:
        at = left.index(bit)
        part = halve(jnp.moveaxis(part, at, 0), bit, replicas)
        left.remove(bit)
    return part


def shards(tokens, cotangent, expert_ids, combine, w_gate, w_up, w_down):
    groups = lax.axis_size("expert")
    replicas = lax.axis_size("dp")
    here = lax.axis_index("expert")
    tok_rows, top = expert_ids.shape
    f32, bf16 = jnp.float32, jnp.bfloat16
    w_gate, w_up, w_down = w_gate[0], w_up[0], w_down[0]

    named = expert_ids[:, :, None] == jnp.arange(groups, dtype=jnp.int32)
    weights = jnp.sum(jnp.where(named, combine[:, :, None], 0.0), axis=1).T
    c_blocks = [lax.dynamic_index_in_dim(weights, here, 0, keepdims=False)]
    for k in range(1, groups):
        shift = [(i, (i + k) % groups) for i in range(groups)]
        row = lax.dynamic_index_in_dim(weights, lax.rem(here + k, groups), 0, keepdims=False)
        c_blocks.append(lax.ppermute(row, "expert", shift))
    c_all = jnp.concatenate(c_blocks)
    x_all = jnp.concatenate(ring_blocks(tokens, groups), axis=0)
    dy_all = jnp.concatenate(ring_blocks(cotangent, groups), axis=0)

    gate = jnp.dot(x_all, w_gate, preferred_element_type=f32)
    up = jnp.dot(x_all, w_up, preferred_element_type=f32)
    sig = jax.nn.sigmoid(gate)
    act = gate * sig
    hidden = (act * up).astype(bf16)
    raw = lax.dot_general(dy_all, w_down, LAST, preferred_element_type=f32)
    comb = jnp.sum(hidden.astype(f32) * raw, axis=1)
    hidden_grad = c_all[:, None] * raw
    gate_d = (hidden_grad * up * (sig * (1.0 + gate * (1.0 - sig)))).astype(bf16)
    up_d = (hidden_grad * act).astype(bf16)
    weighted = (c_all[:, None] * hidden.astype(f32)).astype(bf16)

    bits = replicas.bit_length() - 1
    forward = [0] + list(range(1, bits))
    backward = [0] + list(range(bits - 1, 0, -1))
    down_part = lax.dot_general(weighted, dy_all, FIRST, preferred_element_type=f32).astype(bf16)
    gate_part = lax.dot_general(x_all, gate_d, FIRST, preferred_element_type=f32).astype(bf16)
    up_part = lax.dot_general(x_all, up_d, FIRST, preferred_element_type=f32).astype(bf16)
    half = down_part.shape[1] // 2
    down_grad = jnp.concatenate(
        [
            scatter_sum(down_part[:, :half], forward, replicas),
            scatter_sum(down_part[:, half:], backward, replicas),
        ],
        axis=1,
    )
    gate_grad = scatter_sum(gate_part, forward, replicas)
    up_grad = scatter_sum(up_part, backward, replicas)

    row_grad = lax.dot_general(gate_d, w_gate, LAST, preferred_element_type=f32)
    row_grad = row_grad + lax.dot_general(up_d, w_up, LAST, preferred_element_type=f32)
    row_grad = row_grad.astype(bf16).reshape(groups, tok_rows, -1)
    ring = [(i, (i + 1) % groups) for i in range(groups)]
    total = row_grad[1]
    for k in range(2, groups + 1):
        got = lax.ppermute(total, "expert", ring)
        total = (row_grad[k % groups].astype(f32) + got.astype(f32)).astype(bf16)
    input_grad = total

    comb = comb.reshape(groups, tok_rows)
    mine = jnp.arange(groups)
    columns = [jnp.where((mine == here)[:, None], comb[0], 0.0)]
    for k in range(1, groups):
        shift = [(i, (i - k) % groups) for i in range(groups)]
        got = lax.ppermute(comb[k], "expert", shift)
        columns.append(jnp.where((mine == lax.rem(here + k, groups))[:, None], got, 0.0))
    comb_home = sum(columns).T
    combine_grad = jnp.sum(jnp.where(named, comb_home[:, None, :], 0.0), axis=2)
    return (input_grad, combine_grad, gate_grad[None], up_grad[None], down_grad[None])


def solution(mesh):
    rows = P(("dp", "expert"), None)
    expert = P("expert", None, None)
    return jax.shard_map(
        shards,
        mesh=mesh,
        in_specs=(rows, rows, rows, rows, expert, expert, expert),
        out_specs=(rows, rows, P("expert", "dp", None), P("expert", "dp", None), P("expert", "dp", None)),
        check_vma=False,
    )
```
